32 devices in a mesh: rows: 2 (over core), cols: 4 (over y, x), slabs: 4 (over z).
Axes of the slice: x: 2, y: 2, z: 4, core: 2. Of those that a mesh axis runs over, the one named last changes fastest.
Arguments:
- tracer: float32 [8, 256, 384, 128], P('rows', 'cols', 'slabs'), may hold values from 0.2 to 1.8
- crowding: float32 [8, 256, 384, 128], P('rows', 'cols', 'slabs'), may hold values from 0.5 to 2
Outputs:
- tracer_end: float32 [8, 256, 384, 128], P('rows', 'cols', 'slabs')
The draws below stay inside these ranges and needn't reach their ends.
All inputs are finite; a program needn't handle non-finite values.
Results may differ from the reference program's by a relative error of at most 0.00002.
Values sent between devices are 32-bit elements.
A program may use at most 448 MiB of HBM per device.

```python
import jax
import jax.numpy as jnp
from jax import lax

GRID_Y = 8
GRID_X = 256
GRID_Z = 384
SPECIES = 128
STEPS = 4


def block_levels(key, shape, cuts, smallest, top_value):
    loudness = 1.0
    for dim, shards_of in cuts:
        steps = jax.random.uniform(jax.random.fold_in(jax.random.fold_in(key, 6), dim), (shards_of,), jnp.float32, smallest / len(cuts), top_value / len(cuts))
        loudness = loudness * jnp.repeat(jnp.exp(steps), shape[dim] // shards_of).reshape((-1,) + (1,) * (len(shape) - 1 - dim))
    return loudness


def setup_inputs(seed: int = 0) -> dict:
    key_of = jax.random.split(jax.random.key(seed), 3)
    return {
        "tracer": jnp.clip(0.2 + 1.5999999 * jax.random.uniform(key_of[0], (GRID_Y, GRID_X, GRID_Z, SPECIES), jnp.float32) ** block_levels(key_of[0], (GRID_Y, GRID_X, GRID_Z, SPECIES), ((0, 2), (1, 4), (2, 4)), -0.2, 0.2), 0.2, 1.8),
        "crowding": jnp.clip(0.5 + 1.5 * jax.random.uniform(key_of[1], (GRID_Y, GRID_X, GRID_Z, SPECIES), jnp.float32) ** block_levels(key_of[1], (GRID_Y, GRID_X, GRID_Z, SPECIES), ((0, 2), (1, 4), (2, 4)), -0.2, 0.2), 0.5, 2.0),
    }


def inner_cells(values, dims):
    for dim in dims:
        values = lax.slice_in_dim(values, 1, values.shape[dim] - 1, axis=dim)
    return values


def side_cells(values, dim, start, dims):
    others = [other for other in dims if other != dim]
    values = inner_cells(values, others)
    return lax.slice_in_dim(values, start, start + values.shape[dim] - 2, axis=dim)


def advance(padded, crowding):
    middle = inner_cells(padded, (0, 1, 2))
    lower = [side_cells(padded, dim, 0, (0, 1, 2)) for dim in (0, 1, 2)]
    upper = [side_cells(padded, dim, 2, (0, 1, 2)) for dim in (0, 1, 2)]
    spread = lower[0] + upper[0] + lower[1] + upper[1] + lower[2] + upper[2] - 6.0 * middle
    return middle + 0.1 * spread + 0.2 * middle * (1.0 - middle * crowding)


def reference(tracer, crowding):
    for step in range(STEPS):
        tracer = advance(jnp.pad(tracer, ((1, 1), (1, 1), (1, 1), (0, 0)), mode="constant"), crowding)
    return tracer
```

```python
import functools

import jax
import jax.numpy as jnp
from jax import lax
from jax.experimental import pallas as pl
from jax.experimental.pallas import tpu as pltpu
from jax.sharding import PartitionSpec as P

STEPS = 4
EDGE = 4
MIDDLE = 8
PAD = 8
MESH = pl.DeviceIdType.MESH
AXES = ("rows", "cols", "slabs")


def kernel(sizes, chunks, tracer, crowding, out, field, limit, load_sem, store_sem,
           y_send, y_recv, z_send, z_recv, x_send, x_recv):
    rows, width, depth, species = tracer.shape
    last = chunks - 1
    place = {axis: lax.axis_index(axis) for axis in AXES}
    has = {(axis, side): (place[axis] > 0) if side == 0 else (place[axis] < sizes[axis] - 1)
           for axis in AXES for side in (0, 1)}
    near = {(axis, side): {axis: jnp.clip(place[axis] + 2 * side - 1, 0, sizes[axis] - 1)}
            for axis in AXES for side in (0, 1)}

    def span(k):
        if isinstance(k, int):
            if k == 0:
                return 0, EDGE
            if k == last:
                return width - EDGE, EDGE
        return EDGE + (k - 1) * MIDDLE, MIDDLE

    def face(axis, side, p, k, from_input, to):
        start, count = span(k)
        at, cells = pl.ds(PAD, depth), pl.ds(1 + start, count)
        other = 1 - side
        if axis == "rows":
            src = (tracer.at[side * (rows - 1), pl.ds(start, count)] if from_input
                   else field.at[p, 1 + side * (rows - 1), cells, at])
            dst = field.at[p, other * (rows + 1), cells, at]
            send, recv = y_send.at[p, side, k], y_recv.at[p, other, k]
        elif axis == "slabs":
            src = (tracer.at[:, pl.ds(start, count), pl.ds(side * (depth - 1), 1)] if from_input
                   else field.at[p, pl.ds(1, rows), cells, pl.ds(PAD + side * (depth - 1), 1)])
            dst = field.at[p, pl.ds(1, rows), cells, pl.ds(PAD - 1 + other * (depth + 1), 1)]
            send, recv = z_send.at[p, side, k], z_recv.at[p, other, k]
        else:
            src = (tracer.at[:, side * (width - 1)] if from_input
                   else field.at[p, pl.ds(1, rows), 1 + side * (width - 1), at])
            dst = field.at[p, pl.ds(1, rows), other * (width + 1), at]
            send, recv = x_send.at[p, side], x_recv.at[p, other]
        return pltpu.make_async_remote_copy(
            src_ref=src, dst_ref=dst, send_sem=send, recv_sem=recv,
            device_id=near[axis, to], device_id_type=MESH)

    def each(axes, action):
        for axis in axes:
            for side in (0, 1):
                pl.when(has[axis, side])(functools.partial(action, axis, side))

    def send(axes, p, k, from_input=False):
        each(axes, lambda axis, side: face(axis, side, p, k, from_input, side).start())

    def sent(axes, p, k):
        each(axes, lambda axis, side: face(axis, side, p, k, False, side).wait_send())

    def received(axes, p, k):
        each(axes, lambda axis, side: face(axis, 1 - side, p, k, False, side).wait_recv())

    def load(which, k):
        start, count = span(k)
        if which == 0:
            return pltpu.make_async_copy(
                tracer.at[:, pl.ds(start, count)],
                field.at[0, pl.ds(1, rows), pl.ds(1 + start, count), pl.ds(PAD, depth)],
                load_sem.at[0, k])
        return pltpu.make_async_copy(
            crowding.at[:, pl.ds(start, count)], limit.at[:, pl.ds(start, count)], load_sem.at[1, k])

    def store(p, k):
        start, count = span(k)
        return pltpu.make_async_copy(
            field.at[p, pl.ds(1, rows), pl.ds(1 + start, count), pl.ds(PAD, depth)],
            out.at[:, pl.ds(start, count)], store_sem.at[k])

    barrier = pltpu.get_barrier_semaphore()
    each(AXES, lambda axis, side: pl.semaphore_signal(
        barrier, inc=1, device_id=near[axis, side], device_id_type=MESH))
    for k in range(chunks):
        load(0, k).start()
        load(1, k).start()
    pl.semaphore_wait(barrier, sum(jnp.where(has[key], 1, 0) for key in has))

    send(("cols",), 0, 0, True)
    for k in [*range(1, last), 0, last]:
        send(("rows", "slabs"), 0, k, True)

    def clear(axis, side):
        @pl.when(jnp.logical_not(has[axis, side]))
        def _():
            for p in (0, 1):
                if axis == "rows":
                    @pl.loop(1, width + 1)
                    def _(x):
                        field[p, side * (rows + 1), x, pl.ds(PAD, depth)] = jnp.zeros((depth, species), jnp.float32)
                elif axis == "cols":
                    @pl.loop(1, rows + 1)
                    def _(y):
                        field[p, y, side * (width + 1), pl.ds(PAD, depth)] = jnp.zeros((depth, species), jnp.float32)
                else:
                    @pl.loop(1, width + 1)
                    def _(x):
                        for y in range(1, rows + 1):
                            field[p, y, x, pl.ds(PAD - 1 + side * (depth + 1), 1)] = jnp.zeros((1, species), jnp.float32)

    for axis in AXES:
        for side in (0, 1):
            clear(axis, side)

    def advance(step, k):
        p = step % 2
        start, count = span(k)
        scale = 0.2 if step == 0 else 0.05 if step == STEPS - 1 else 0.1

        @pl.loop(0, depth // 8)
        def _(tile):
            at = pl.multiple_of(PAD + tile * 8, 8)
            source = pl.multiple_of(tile * 8, 8)

            def cell(y, x, shift=0):
                return field[p, y, 1 + start + x, pl.ds(at + shift, 8)]

            before = [cell(y, -1) for y in range(1, rows + 1)]
            here = [cell(y, 0) for y in range(1, rows + 1)]
            for x in range(count):
                after = [cell(y, x + 1) for y in range(1, rows + 1)]
                column = [cell(0, x), *here, cell(rows + 1, x)]
                for y in range(rows):
                    middle = here[y]
                    around = (before[y] + after[y]) + (column[y] + column[y + 2])
                    around = around + (cell(y + 1, x, -1) + cell(y + 1, x, 1))
                    bound = limit[y, start + x, pl.ds(source, 8)]
                    if step == 0:
                        bound = bound + bound
                    field[1 - p, y + 1, 1 + start + x, pl.ds(at, 8)] = scale * (around + middle * (6.0 - bound * middle))
                before, here = here, after

    def chunk(step, k, edge):
        p = step % 2
        axes = AXES if edge else ("rows", "slabs")
        if step == 0:
            load(1, k).wait()
            if not edge:
                pl.when(k < last - 1)(lambda: load(0, k + 1).wait())
                pl.when(k == last - 1)(lambda: load(0, last).wait())
        both = ("rows", "slabs")
        received(both, p, k)
        if step >= 1:
            sent(both, 1 - p, k)
        if edge:
            side = 0 if k == 0 else 1
            one = lambda action: pl.when(has["cols", side])(action)
            one(lambda: face("cols", 1 - side, p, k, False, side).wait_recv())
            if step >= 1:
                one(lambda: face("cols", side, 1 - p, k, False, side).wait_send())
        advance(step, k)
        if step < STEPS - 1:
            if edge:
                one(lambda: face("cols", side, 1 - p, k, False, side).start())
            send(both, 1 - p, k)
        else:
            store(1 - p, k).start()

    for step in range(STEPS):
        if step == 0:
            load(0, 0).wait()
            load(0, 1).wait()

        @pl.loop(1, last)
        def _(k):
            chunk(step, k, False)

        chunk(step, 0, True)
        chunk(step, last, True)

    p = (STEPS - 1) % 2

    @pl.loop(1, last)
    def _(k):
        sent(("rows", "slabs"), p, k)
        store(1 - p, k).wait()

    for k in (0, last):
        sent(("rows", "slabs"), p, k)
        store(1 - p, k).wait()
    sent(("cols",), p, 0)


def solution(mesh):
    sizes = dict(mesh.shape)

    def on_device(tracer, crowding):
        rows, width, depth, species = tracer.shape
        chunks = (width - 2 * EDGE) // MIDDLE + 2
        dma = pltpu.SemaphoreType.DMA
        return pl.pallas_call(
            functools.partial(kernel, sizes, chunks),
            out_shape=jax.ShapeDtypeStruct(tracer.shape, jnp.float32),
            in_specs=[pl.BlockSpec(memory_space=pl.ANY)] * 2,
            out_specs=pl.BlockSpec(memory_space=pl.ANY),
            scratch_shapes=[
                pltpu.VMEM((2, rows + 2, width + 2, depth + 2 * PAD, species), jnp.float32),
                pltpu.VMEM(tracer.shape, jnp.float32),
                dma((2, chunks)), dma((chunks,)),
                dma((2, 2, chunks)), dma((2, 2, chunks)),
                dma((2, 2, chunks)), dma((2, 2, chunks)),
                dma((2, 2)), dma((2, 2)),
            ],
            compiler_params=pltpu.CompilerParams(
                collective_id=0, has_side_effects=True, vmem_limit_bytes=67043328),
        )(tracer, crowding)

    return jax.shard_map(
        on_device, mesh=mesh,
        in_specs=(P("rows", "cols", "slabs", None), P("rows", "cols", "slabs", None)),
        out_specs=P("rows", "cols", "slabs", None), check_vma=False)
```

```python
import functools

import jax
import jax.numpy as jnp
from jax import lax
from jax.experimental import pallas as pl
from jax.experimental.pallas import tpu as pltpu
from jax.sharding import PartitionSpec as P

STEPS = 4
EDGE = 4
MIDDLE = 8
PAD = 8
VMEM_LIMIT = 40 * 1024 * 1024
MESH = pl.DeviceIdType.MESH
AXES = ("rows", "cols", "slabs")


class Levels:
    def __init__(self, *refs):
        self.refs = refs

    @property
    def at(self):
        return self

    def __getitem__(self, index):
        return self.refs[index[0]].at[index[1:]]


def write(ended, out, store_sem):
    rows, width, depth, species = out.shape
    copies = [pltpu.make_async_copy(
        ended.at[1 + y, pl.ds(1, width), pl.ds(PAD, depth)], out.at[y], store_sem.at[y])
        for y in range(rows)]
    for copy in copies:
        copy.start()
    for copy in copies:
        copy.wait()


def kernel(sizes, chunks, tracer, crowding, ended, other_field, limit, load_sem,
           y_send, y_recv, z_send, z_recv, x_send, x_recv):
    rows, width, depth, species = tracer.shape
    last = chunks - 1
    field = Levels(ended, other_field)
    place = {axis: lax.axis_index(axis) for axis in AXES}
    has = {(axis, side): (place[axis] > 0) if side == 0 else (place[axis] < sizes[axis] - 1)
           for axis in AXES for side in (0, 1)}
    near = {(axis, side): {axis: jnp.clip(place[axis] + 2 * side - 1, 0, sizes[axis] - 1)}
            for axis in AXES for side in (0, 1)}

    def span(k):
        if isinstance(k, int):
            if k == 0:
                return 0, EDGE
            if k == last:
                return width - EDGE, EDGE
        return EDGE + (k - 1) * MIDDLE, MIDDLE

    def face(axis, side, p, k, from_input, to):
        start, count = span(k)
        at, cells = pl.ds(PAD, depth), pl.ds(1 + start, count)
        other = 1 - side
        if axis == "rows":
            src = (tracer.at[side * (rows - 1), pl.ds(start, count)] if from_input
                   else field.at[p, 1 + side * (rows - 1), cells, at])
            dst = field.at[p, other * (rows + 1), cells, at]
            send, recv = y_send.at[p, side, k], y_recv.at[p, other, k]
        elif axis == "slabs":
            src = (tracer.at[:, pl.ds(start, count), pl.ds(side * (depth - 1), 1)] if from_input
                   else field.at[p, pl.ds(1, rows), cells, pl.ds(PAD + side * (depth - 1), 1)])
            dst = field.at[p, pl.ds(1, rows), cells, pl.ds(PAD - 1 + other * (depth + 1), 1)]
            send, recv = z_send.at[p, side, k], z_recv.at[p, other, k]
        else:
            src = (tracer.at[:, side * (width - 1)] if from_input
                   else field.at[p, pl.ds(1, rows), 1 + side * (width - 1), at])
            dst = field.at[p, pl.ds(1, rows), other * (width + 1), at]
            send, recv = x_send.at[p, side], x_recv.at[p, other]
        return pltpu.make_async_remote_copy(
            src_ref=src, dst_ref=dst, send_sem=send, recv_sem=recv,
            device_id=near[axis, to], device_id_type=MESH)

    def each(axes, action):
        for axis in axes:
            for side in (0, 1):
                pl.when(has[axis, side])(functools.partial(action, axis, side))

    def send(axes, p, k, from_input=False):
        each(axes, lambda axis, side: face(axis, side, p, k, from_input, side).start())

    def sent(axes, p, k):
        each(axes, lambda axis, side: face(axis, side, p, k, False, side).wait_send())

    def received(axes, p, k):
        each(axes, lambda axis, side: face(axis, 1 - side, p, k, False, side).wait_recv())

    def load(which, k):
        start, count = span(k)
        if which == 0:
            return pltpu.make_async_copy(
                tracer.at[:, pl.ds(start, count)],
                field.at[0, pl.ds(1, rows), pl.ds(1 + start, count), pl.ds(PAD, depth)],
                load_sem.at[0, k])
        return pltpu.make_async_copy(
            crowding.at[:, pl.ds(start, count)], limit.at[:, pl.ds(start, count)], load_sem.at[1, k])

    barrier = pltpu.get_barrier_semaphore()
    each(AXES, lambda axis, side: pl.semaphore_signal(
        barrier, inc=1, device_id=near[axis, side], device_id_type=MESH))
    for k in range(chunks):
        load(0, k).start()
        load(1, k).start()
    pl.semaphore_wait(barrier, sum(jnp.where(has[key], 1, 0) for key in has))

    send(("cols",), 0, 0, True)
    for k in [*range(1, last), 0, last]:
        send(("rows", "slabs"), 0, k, True)

    def clear(axis, side):
        @pl.when(jnp.logical_not(has[axis, side]))
        def _():
            for p in (0, 1):
                if axis == "rows":
                    @pl.loop(1, width + 1)
                    def _(x):
                        field.refs[p][side * (rows + 1), x, pl.ds(PAD, depth)] = jnp.zeros((depth, species), jnp.float32)
                elif axis == "cols":
                    @pl.loop(1, rows + 1)
                    def _(y):
                        field.refs[p][y, side * (width + 1), pl.ds(PAD, depth)] = jnp.zeros((depth, species), jnp.float32)
                else:
                    @pl.loop(1, width + 1)
                    def _(x):
                        for y in range(1, rows + 1):
                            field.refs[p][y, x, pl.ds(PAD - 1 + side * (depth + 1), 1)] = jnp.zeros((1, species), jnp.float32)

    for axis in AXES:
        for side in (0, 1):
            clear(axis, side)

    def advance(step, k):
        p = step % 2
        start, count = span(k)
        scale = 0.2 if step == 0 else 0.05 if step == STEPS - 1 else 0.1

        @pl.loop(0, depth // 8)
        def _(tile):
            at = pl.multiple_of(PAD + tile * 8, 8)
            source = pl.multiple_of(tile * 8, 8)

            def cell(y, x, shift=0):
                return field.refs[p][y, 1 + start + x, pl.ds(at + shift, 8)]

            before = [cell(y, -1) for y in range(1, rows + 1)]
            here = [cell(y, 0) for y in range(1, rows + 1)]
            for x in range(count):
                after = [cell(y, x + 1) for y in range(1, rows + 1)]
                column = [cell(0, x), *here, cell(rows + 1, x)]
                for y in range(rows):
                    middle = here[y]
                    around = (before[y] + after[y]) + (column[y] + column[y + 2])
                    around = around + (cell(y + 1, x, -1) + cell(y + 1, x, 1))
                    bound = limit[y, start + x, pl.ds(source, 8)]
                    if step == 0:
                        bound = bound + bound
                    field.refs[1 - p][y + 1, 1 + start + x, pl.ds(at, 8)] = scale * (around + middle * (6.0 - bound * middle))
                before, here = here, after

    def chunk(step, k, edge):
        p = step % 2
        axes = AXES if edge else ("rows", "slabs")
        if step == 0:
            load(1, k).wait()
            if not edge:
                pl.when(k < last - 1)(lambda: load(0, k + 1).wait())
                pl.when(k == last - 1)(lambda: load(0, last).wait())
        both = ("rows", "slabs")
        received(both, p, k)
        if step >= 1:
            sent(both, 1 - p, k)
        if edge:
            side = 0 if k == 0 else 1
            one = lambda action: pl.when(has["cols", side])(action)
            one(lambda: face("cols", 1 - side, p, k, False, side).wait_recv())
            if step >= 1:
                one(lambda: face("cols", side, 1 - p, k, False, side).wait_send())
        advance(step, k)
        if step < STEPS - 1:
            if edge:
                one(lambda: face("cols", side, 1 - p, k, False, side).start())
            send(both, 1 - p, k)

    for step in range(STEPS):
        if step == 0:
            load(0, 0).wait()
            load(0, 1).wait()

        @pl.loop(1, last)
        def _(k):
            chunk(step, k, False)

        chunk(step, 0, True)
        chunk(step, last, True)

    p = (STEPS - 1) % 2

    @pl.loop(1, last)
    def _(k):
        sent(("rows", "slabs"), p, k)

    for k in (0, last):
        sent(("rows", "slabs"), p, k)
    sent(("cols",), p, 0)


def solution(mesh):
    sizes = dict(mesh.shape)

    def on_device(tracer, crowding):
        rows, width, depth, species = tracer.shape
        chunks = (width - 2 * EDGE) // MIDDLE + 2
        dma = pltpu.SemaphoreType.DMA
        padded = (rows + 2, width + 2, depth + 2 * PAD, species)
        cell_count = rows * width * depth * species
        ended = pl.pallas_call(
            functools.partial(kernel, sizes, chunks),
            out_shape=pltpu.VMEM(padded, jnp.float32),
            in_specs=[pl.BlockSpec(memory_space=pl.ANY)] * 2,
            out_specs=pl.BlockSpec(memory_space=pltpu.VMEM),
            scratch_shapes=[
                pltpu.VMEM(padded, jnp.float32),
                pltpu.VMEM(tracer.shape, jnp.float32),
                dma((2, chunks)),
                dma((2, 2, chunks)), dma((2, 2, chunks)),
                dma((2, 2, chunks)), dma((2, 2, chunks)),
                dma((2, 2)), dma((2, 2)),
            ],
            compiler_params=pltpu.CompilerParams(
                collective_id=0, has_side_effects=True, vmem_limit_bytes=VMEM_LIMIT),
        )(tracer, crowding)
        return pl.pallas_call(
            write,
            out_shape=jax.ShapeDtypeStruct(tracer.shape, jnp.float32),
            in_specs=[pl.BlockSpec(memory_space=pltpu.VMEM)],
            out_specs=pl.BlockSpec(memory_space=pl.ANY),
            scratch_shapes=[dma((rows,))],
            compiler_params=pltpu.CompilerParams(vmem_limit_bytes=1 << 20),
        )(ended)

    return jax.shard_map(
        on_device, mesh=mesh,
        in_specs=(P("rows", "cols", "slabs", None), P("rows", "cols", "slabs", None)),
        out_specs=P("rows", "cols", "slabs", None), check_vma=False)
```

```python
import functools

import jax
import jax.numpy as jnp
from jax import lax
from jax.experimental import pallas as pl
from jax.experimental.pallas import tpu as pltpu
from jax.sharding import PartitionSpec as P

STEPS = 4
EDGE = 2
VIA = {1: 3, 2: 0}
GAP = 1
LATE = 3
RELAYED = 1
MIDDLE = 10
PAD = 8
VMEM_LIMIT = 40 * 1024 * 1024
MESH = pl.DeviceIdType.MESH
AXES = ("rows", "cols", "slabs")


class Levels:
    def __init__(self, *refs):
        self.refs = refs

    @property
    def at(self):
        return self

    def __getitem__(self, index):
        return self.refs[index[0]].at[index[1:]]


def write(ended, out, store_sem):
    rows, width, depth, species = out.shape
    copies = [pltpu.make_async_copy(
        ended.at[1 + y, pl.ds(1, width), pl.ds(PAD, depth)], out.at[y], store_sem.at[y])
        for y in range(rows)]
    for copy in copies:
        copy.start()
    for copy in copies:
        copy.wait()


def kernel(sizes, chunks, via, tracer, crowding, ended, other_field, limit, load_sem,
           y_send, y_recv, z_send, z_recv, x_send, x_recv,
           relayed, r_send, r_recv, f_send, f_recv):
    rows, width, depth, species = tracer.shape
    last = chunks - 1
    field = Levels(ended, other_field)
    place = {axis: lax.axis_index(axis) for axis in AXES}
    has = {(axis, side): (place[axis] > 0) if side == 0 else (place[axis] < sizes[axis] - 1)
           for axis in AXES for side in (0, 1)}
    near = {(axis, side): {axis: jnp.clip(place[axis] + 2 * side - 1, 0, sizes[axis] - 1)}
            for axis in AXES for side in (0, 1)}

    col = place["cols"]
    direct = rows - min(RELAYED, rows // 2) if via else rows

    def span(k):
        if isinstance(k, int):
            if k == 0:
                return 0, EDGE
            if k == last:
                return width - EDGE, EDGE
        return EDGE + (k - 1) * MIDDLE, MIDDLE

    def face(axis, side, p, k, from_input, to, part=rows):
        start, count = span(k)
        at, cells = pl.ds(PAD, depth), pl.ds(1 + start, count)
        other = 1 - side
        if axis == "rows":
            src = (tracer.at[side * (rows - 1), pl.ds(start, count)] if from_input
                   else field.at[p, 1 + side * (rows - 1), cells, at])
            dst = field.at[p, other * (rows + 1), cells, at]
            send, recv = y_send.at[p, side, k], y_recv.at[p, other, k]
        elif axis == "slabs":
            src = (tracer.at[:, pl.ds(start, count), pl.ds(side * (depth - 1), 1)] if from_input
                   else field.at[p, pl.ds(1, rows), cells, pl.ds(PAD + side * (depth - 1), 1)])
            dst = field.at[p, pl.ds(1, rows), cells, pl.ds(PAD - 1 + other * (depth + 1), 1)]
            send, recv = z_send.at[p, side, k], z_recv.at[p, other, k]
        else:
            src = (tracer.at[pl.ds(0, part), side * (width - 1)] if from_input
                   else field.at[p, pl.ds(1, part), 1 + side * (width - 1), at])
            dst = field.at[p, pl.ds(1, part), other * (width + 1), at]
            send, recv = x_send.at[p, side], x_recv.at[p, other]
        return pltpu.make_async_remote_copy(
            src_ref=src, dst_ref=dst, send_sem=send, recv_sem=recv,
            device_id=near[axis, to], device_id_type=MESH)

    def x_face(side, to, p, from_input, action):
        if not via:
            pl.when(has["cols", to])(lambda: action(face("cols", side, p, 0, from_input, to)))
            return
        long = col == 2 - to
        pl.when(long)(lambda: action(face("cols", side, p, 0, from_input, to, direct)))
        pl.when(jnp.logical_and(has["cols", to], jnp.logical_not(long)))(
            lambda: action(face("cols", side, p, 0, from_input, to)))

    def first_hop(source, event, row, from_input):
        side = 2 - source
        src = (tracer.at[direct + row, side * (width - 1)] if from_input
               else field.at[event % 2, 1 + direct + row, 1 + side * (width - 1), pl.ds(PAD, depth)])
        return pltpu.make_async_remote_copy(
            src_ref=src, dst_ref=relayed.at[event, row],
            send_sem=r_send.at[event, row], recv_sem=r_recv.at[event, row],
            device_id={"cols": via[source]}, device_id_type=MESH)

    def second_hop(source, event, row):
        side = 2 - source
        return pltpu.make_async_remote_copy(
            src_ref=relayed.at[event, row],
            dst_ref=field.at[event % 2, 1 + direct + row, (1 - side) * (width + 1), pl.ds(PAD, depth)],
            send_sem=f_send.at[event, row], recv_sem=f_recv.at[event, row],
            device_id={"cols": 3 - source}, device_id_type=MESH)

    def hops(action, *who):
        if via:
            for source in (1, 2):
                @pl.when(col == who[source - 1])
                def _():
                    for row in range(rows - direct):
                        action(source, row)

    def in_order(action):
        def both(*sides):
            for side in sides:
                action(side)

        if via:
            pl.when(col == 1)(lambda: both(1, 0))
            pl.when(col != 1)(lambda: both(0, 1))
        else:
            both(0, 1)

    def pass_on(event, row):
        for source in (1, 2):
            @pl.when(col == via[source])
            def _():
                first_hop(source, event, row, False).wait_recv()
                second_hop(source, event, row).start()

    def each(axes, action):
        for axis in axes:
            for side in (0, 1):
                pl.when(has[axis, side])(functools.partial(action, axis, side))

    def send(axes, p, k, from_input=False):
        each(axes, lambda axis, side: face(axis, side, p, k, from_input, side).start())

    def sent(axes, p, k):
        each(axes, lambda axis, side: face(axis, side, p, k, False, side).wait_send())

    def received(axes, p, k):
        each(axes, lambda axis, side: face(axis, 1 - side, p, k, False, side).wait_recv())

    def load(which, k):
        start, count = span(k)
        if which == 0:
            return pltpu.make_async_copy(
                tracer.at[:, pl.ds(start, count)],
                field.at[0, pl.ds(1, rows), pl.ds(1 + start, count), pl.ds(PAD, depth)],
                load_sem.at[0, k])
        return pltpu.make_async_copy(
            crowding.at[:, pl.ds(start, count)], limit.at[:, pl.ds(start, count)], load_sem.at[1, k])

    barrier = pltpu.get_barrier_semaphore()
    each(AXES, lambda axis, side: pl.semaphore_signal(
        barrier, inc=1, device_id=near[axis, side], device_id_type=MESH))
    for k in range(chunks):
        load(0, k).start()
        load(1, k).start()
    if via:
        pl.semaphore_signal(barrier, inc=1, device_id={"cols": lax.rem(col + 2, 4)}, device_id_type=MESH)
    pl.semaphore_wait(barrier, (1 if via else 0) + sum(jnp.where(has[key], 1, 0) for key in has))

    hops(lambda source, row: first_hop(source, 0, row, True).start(), 1, 2)
    in_order(lambda side: x_face(side, side, 0, True, lambda copy: copy.start()))
    for k in [*range(1, last), 0, last]:
        send(("rows", "slabs"), 0, k, True)

    def clear(axis, side):
        @pl.when(jnp.logical_not(has[axis, side]))
        def _():
            for p in (0, 1):
                if axis == "rows":
                    @pl.loop(1, width + 1)
                    def _(x):
                        field.refs[p][side * (rows + 1), x, pl.ds(PAD, depth)] = jnp.zeros((depth, species), jnp.float32)
                elif axis == "cols":
                    @pl.loop(1, rows + 1)
                    def _(y):
                        field.refs[p][y, side * (width + 1), pl.ds(PAD, depth)] = jnp.zeros((depth, species), jnp.float32)
                else:
                    @pl.loop(1, width + 1)
                    def _(x):
                        for y in range(1, rows + 1):
                            field.refs[p][y, x, pl.ds(PAD - 1 + side * (depth + 1), 1)] = jnp.zeros((1, species), jnp.float32)

    for axis in AXES:
        for side in (0, 1):
            clear(axis, side)

    def advance(step, k):
        p = step % 2
        start, count = span(k)
        scale = 0.2 if step == 0 else 0.05 if step == STEPS - 1 else 0.1

        @pl.loop(0, depth // 8)
        def _(tile):
            at = pl.multiple_of(PAD + tile * 8, 8)
            source = pl.multiple_of(tile * 8, 8)

            def cell(y, x, shift=0):
                return field.refs[p][y, 1 + start + x, pl.ds(at + shift, 8)]

            before = [cell(y, -1) for y in range(1, rows + 1)]
            here = [cell(y, 0) for y in range(1, rows + 1)]
            for x in range(count):
                after = [cell(y, x + 1) for y in range(1, rows + 1)]
                column = [cell(0, x), *here, cell(rows + 1, x)]
                for y in range(rows):
                    middle = here[y]
                    around = (before[y] + after[y]) + (column[y] + column[y + 2])
                    around = around + (cell(y + 1, x, -1) + cell(y + 1, x, 1))
                    bound = limit[y, start + x, pl.ds(source, 8)]
                    if step == 0:
                        bound = bound + bound
                    field.refs[1 - p][y + 1, 1 + start + x, pl.ds(at, 8)] = scale * (around + middle * (6.0 - bound * middle))
                before, here = here, after

    def chunk(step, k, edge):
        p = step % 2
        axes = AXES if edge else ("rows", "slabs")
        if step == 0:
            load(1, k).wait()
            if not edge:
                pl.when(k < last - 1)(lambda: load(0, k + 1).wait())
                pl.when(k == last - 1)(lambda: load(0, last).wait())
        both = ("rows", "slabs")
        received(both, p, k)
        if step >= 1:
            sent(both, 1 - p, k)
        if edge:
            side = 0 if k == 0 else 1
            x_face(1 - side, side, p, False, lambda copy: copy.wait_recv())
            if via:
                @pl.when(col == 2 - side)
                def _():
                    for row in range(rows - direct):
                        second_hop(1 + side, step, row).wait_recv()
            if step >= 1:
                x_face(side, side, 1 - p, False, lambda copy: copy.wait_send())
                if via:
                    @pl.when(col == 2 - side)
                    def _():
                        for row in range(rows - direct):
                            first_hop(2 - side, step - 1, row, False).wait_send()
        advance(step, k)
        if step < STEPS - 1:
            if edge:
                if via:
                    @pl.when(col == 2 - side)
                    def _():
                        for row in range(rows - direct):
                            first_hop(2 - side, step + 1, row, False).start()
                x_face(side, side, 1 - p, False, lambda copy: copy.start())
            send(both, 1 - p, k)

    for step in range(STEPS):
        if step == 0:
            load(0, 0).wait()
            load(0, 1).wait()

        @pl.loop(1, last)
        def _(k):
            chunk(step, k, False)
            if via:
                for row in range(rows - direct):
                    pl.when(k == max(1, last - 1 - LATE - GAP * (rows - direct - 1 - row)))(
                        functools.partial(pass_on, step, row))

        in_order(lambda side: chunk(step, side * last, True))

    p = (STEPS - 1) % 2

    @pl.loop(1, last)
    def _(k):
        sent(("rows", "slabs"), p, k)

    for k in (0, last):
        sent(("rows", "slabs"), p, k)
    for side in (0, 1):
        x_face(side, side, p, False, lambda copy: copy.wait_send())
    hops(lambda source, row: first_hop(source, STEPS - 1, row, False).wait_send(), 1, 2)
    for event in range(STEPS):
        hops(lambda source, row: second_hop(source, event, row).wait_send(), *[via[k] for k in (1, 2)] if via else ())


def relays(mesh):
    if mesh.shape["cols"] != 4:
        return None
    devices = mesh.devices.transpose([mesh.axis_names.index(axis) for axis in AXES])[0, :, 0]
    chips = [getattr(device, "coords", None) for device in devices]
    if any(chip is None for chip in chips):
        return None
    apart = sum(a != b for a, b in zip(chips[1], chips[2]))
    return VIA if apart > 1 else None


def solution(mesh):
    sizes = dict(mesh.shape)
    via = relays(mesh)

    def on_device(tracer, crowding):
        rows, width, depth, species = tracer.shape
        chunks = (width - 2 * EDGE) // MIDDLE + 2
        dma = pltpu.SemaphoreType.DMA
        padded = (rows + 2, width + 2, depth + 2 * PAD, species)
        cell_count = rows * width * depth * species
        ended = pl.pallas_call(
            functools.partial(kernel, sizes, chunks, via),
            out_shape=pltpu.VMEM(padded, jnp.float32),
            in_specs=[pl.BlockSpec(memory_space=pl.ANY)] * 2,
            out_specs=pl.BlockSpec(memory_space=pltpu.VMEM),
            scratch_shapes=[
                pltpu.VMEM(padded, jnp.float32),
                pltpu.VMEM(tracer.shape, jnp.float32),
                dma((2, chunks)),
                dma((2, 2, chunks)), dma((2, 2, chunks)),
                dma((2, 2, chunks)), dma((2, 2, chunks)),
                dma((2, 2)), dma((2, 2)),
                pltpu.VMEM((STEPS, max(1, rows // 2), depth, species), jnp.float32),
                *[dma((STEPS, max(1, rows // 2)))] * 4,
            ],
            compiler_params=pltpu.CompilerParams(
                collective_id=0, has_side_effects=True, vmem_limit_bytes=VMEM_LIMIT),
        )(tracer, crowding)
        return pl.pallas_call(
            write,
            out_shape=jax.ShapeDtypeStruct(tracer.shape, jnp.float32),
            in_specs=[pl.BlockSpec(memory_space=pltpu.VMEM)],
            out_specs=pl.BlockSpec(memory_space=pl.ANY),
            scratch_shapes=[dma((rows,))],
            compiler_params=pltpu.CompilerParams(vmem_limit_bytes=1 << 20),
        )(ended)

    return jax.shard_map(
        on_device, mesh=mesh,
        in_specs=(P("rows", "cols", "slabs", None), P("rows", "cols", "slabs", None)),
        out_specs=P("rows", "cols", "slabs", None), check_vma=False)
```
